8 devices in a mesh: dp: 1 (over z), ri: 2 (over y), co: 2 (over x), ro: 2 (over core).
Axes of the slice: x: 2, y: 2, z: 1, core: 2. Of those that a mesh axis runs over, the one named last changes fastest.
Arguments:
- a_mat: bfloat16 [4096, 32768], P(('dp', 'ri', 'ro'), 'co')
- b_mat: bfloat16 [32768, 16384], P(('dp', 'ri', 'ro'), 'co')
Outputs:
- output: bfloat16 [4096, 16384], P(('dp', 'ri', 'ro'), 'co')
All inputs are finite; a program needn't handle non-finite values.
Results may differ from the reference program's by a relative error of at most 0.001.
Values are sent between devices in bfloat16 or wider.
A program may use at most 1 GiB of HBM per device.

```python
import jax
import jax.numpy as jnp

M_ROWS = 4096
N_COLS = 16384
K_DEPTH = 32768


def setup_inputs(seed: int = 0, part: int = 0) -> dict:
    base_key = jax.random.fold_in(jax.random.key(seed), part)
    key_a, key_b = jax.random.split(base_key)
    left_mat = jax.random.normal(key_a, (M_ROWS, K_DEPTH), jnp.float32)
    right_mat = jax.random.normal(key_b, (K_DEPTH, N_COLS), jnp.float32) * (K_DEPTH ** -0.5)
    return {"a_mat": left_mat.astype(jnp.bfloat16), "b_mat": right_mat.astype(jnp.bfloat16)}


def reference(a_mat, b_mat):
    product = jnp.dot(a_mat, b_mat, preferred_element_type=jnp.float32)
    return product.astype(jnp.bfloat16)
```

```python
import functools

import jax
import jax.numpy as jnp
from jax import lax
from jax.experimental import pallas as pl
from jax.experimental.pallas import tpu as pltpu
from jax.sharding import PartitionSpec as P

MESH = pl.DeviceIdType.MESH
UNITS = 4
B_BUFFERS = 3


def make_sizes(rows, k_half, cols):
    k_quarter = k_half // 2
    return dict(
        rows=rows,
        k_half=k_half,
        k_quarter=k_quarter,
        cols=cols,
        unit=rows // UNITS,
        tile=cols // 8,
        x0_depth=k_quarter // 8,
        x1_depth=k_quarter // 4,
    )


def kernel(sizes, a, b, out, b_far, x0, x1, stage, part, acc, far_s, far_r, x0_s, x0_r, x1_s, x1_r, fwd_s, part_s, part_r, b_sem, x_sem, o_sem):
    rows, k_half, k_quarter = sizes["rows"], sizes["k_half"], sizes["k_quarter"]
    unit, tile = sizes["unit"], sizes["tile"]
    n_tiles = sizes["cols"] // tile
    i, j, r = lax.axis_index("ri"), lax.axis_index("co"), lax.axis_index("ro")
    dp = lax.axis_index("dp")
    vertical, horizontal = (dp, 1 - i, j, r), (dp, i, 1 - j, r)
    opposite, partner = (dp, 1 - i, 1 - j, r), (dp, i, j, 1 - r)
    diag = i == j
    off = jnp.logical_not(diag)

    barrier = pltpu.get_barrier_semaphore()
    for device in (vertical, horizontal, opposite, partner):
        pl.semaphore_signal(barrier, inc=1, device_id=device, device_id_type=MESH)
    pl.semaphore_wait(barrier, 4)

    def remote(src, dst, send, recv, device):
        return pltpu.make_async_remote_copy(
            src_ref=src, dst_ref=dst, send_sem=send, recv_sem=recv, device_id=device, device_id_type=MESH
        )

    far_rows = k_quarter // 8

    def far_copy(c):
        block = pl.ds(c * far_rows, far_rows)
        return remote(b.at[block], b_far.at[block], far_s.at[c], far_r.at[c], partner)

    def k_column(kc, depth):
        return pl.multiple_of(lax.rem(r * k_quarter + kc * depth, k_half), depth)

    x0_depth = sizes["x0_depth"]
    n_x0 = k_half // x0_depth

    def x0_copy(kc):
        block = pl.ds(k_column(kc, x0_depth), x0_depth)
        return remote(a.at[:, block], x0.at[:, block], x0_s.at[kc], x0_r.at[kc], horizontal)

    def unit_rows(u):
        return pl.ds(pl.multiple_of(u * unit, unit), unit)

    def x1_send(u, device):
        return remote(a.at[unit_rows(u)], x1.at[unit_rows(u)], x1_s.at[u], x1_r.at[u], device)

    def x1_forward(u):
        return remote(x1.at[unit_rows(u)], x1.at[unit_rows(u)], fwd_s.at[u], x1_r.at[u], horizontal)

    def tile_cols(t):
        return pl.ds(pl.multiple_of(t * tile, tile), tile)

    def part_copy(u, t):
        where = (unit_rows(u), tile_cols(t))
        return remote(stage.at[where], part.at[where], part_s.at[u * n_tiles + t], part_r.at[u * n_tiles + t], vertical)

    def each(n, step):
        def body(c, carry):
            step(c)
            return carry

        lax.fori_loop(0, n, body, 0)

    def own_rows(first, last, source, b_source, ready=None, b_ready=None):
        base = first if first < n_x0 // 2 else first - n_x0 // 2
        steps = (last - first) * n_tiles

        def scope(xbuf, bbuf):
            def b_copy(s):
                c = lax.div(s, n_tiles)
                t = lax.rem(s, n_tiles)
                slot = lax.rem(s, B_BUFFERS)
                k_rows = pl.ds(pl.multiple_of((base + c) * x0_depth, x0_depth), x0_depth)
                return pltpu.make_async_copy(b_source.at[k_rows, tile_cols(t)], bbuf.at[slot], b_sem.at[slot])

            def b_start(s):
                if b_ready is not None:

                    @pl.when(lax.rem(s, n_tiles) == 0)
                    def _():
                        b_ready(base + lax.div(s, n_tiles))

                b_copy(s).start()

            for s in range(B_BUFFERS - 1):
                b_start(jnp.int32(s))

            def body(s, carry):
                c = lax.div(s, n_tiles)
                t = lax.rem(s, n_tiles)

                @pl.when(s + B_BUFFERS - 1 < steps)
                def _():
                    b_start(s + B_BUFFERS - 1)

                @pl.when(t == 0)
                def _():
                    if ready is not None:
                        ready(first + c)
                    block = pl.ds(k_column(first + c, x0_depth), x0_depth)
                    copy = pltpu.make_async_copy(source.at[:, block], xbuf, x_sem)
                    copy.start()
                    copy.wait()

                b_copy(s).wait()
                product = jnp.dot(xbuf[...], bbuf[lax.rem(s, B_BUFFERS)], preferred_element_type=jnp.float32)
                if first == 0:

                    @pl.when(c == 0)
                    def _():
                        acc[:, tile_cols(t)] = product

                    @pl.when(c > 0)
                    def _():
                        acc[:, tile_cols(t)] += product
                else:
                    acc[:, tile_cols(t)] += product
                return carry

            lax.fori_loop(0, steps, body, 0)

        pl.run_scoped(
            scope,
            pltpu.VMEM((rows, x0_depth), jnp.bfloat16),
            pltpu.VMEM((B_BUFFERS, x0_depth, tile), jnp.bfloat16),
        )

    x1_depth = sizes["x1_depth"]
    n_x1 = k_half // x1_depth

    def other_rows(u):
        steps = n_tiles * n_x1

        def scope(xbuf, bbuf, pbuf):
            def b_start(s):
                t = lax.div(s, n_x1)
                kc = lax.rem(s, n_x1)
                slot = lax.rem(s, B_BUFFERS)

                @pl.when(kc < n_x1 // 2)
                def _():
                    k_rows = pl.ds(pl.multiple_of(kc * x1_depth, x1_depth), x1_depth)
                    pltpu.make_async_copy(b.at[k_rows, tile_cols(t)], bbuf.at[slot], b_sem.at[slot]).start()

                @pl.when(kc >= n_x1 // 2)
                def _():
                    k_rows = pl.ds(pl.multiple_of((kc - n_x1 // 2) * x1_depth, x1_depth), x1_depth)
                    pltpu.make_async_copy(b_far.at[k_rows, tile_cols(t)], bbuf.at[slot], b_sem.at[slot]).start()

            load = pltpu.make_async_copy(x1.at[unit_rows(u)], xbuf, x_sem)
            load.start()
            for s in range(B_BUFFERS - 1):
                b_start(jnp.int32(s))
            load.wait()

            def body(s, carry):
                t = lax.div(s, n_x1)
                kc = lax.rem(s, n_x1)
                slot = lax.rem(s, B_BUFFERS)

                @pl.when(s + B_BUFFERS - 1 < steps)
                def _():
                    b_start(s + B_BUFFERS - 1)

                pltpu.make_async_copy(b.at[pl.ds(0, x1_depth), pl.ds(0, tile)], bbuf.at[slot], b_sem.at[slot]).wait()
                columns = pl.ds(k_column(kc, x1_depth), x1_depth)
                product = jnp.dot(xbuf[:, columns], bbuf[slot], preferred_element_type=jnp.float32)

                @pl.when(kc == 0)
                def _():
                    pbuf[...] = product

                @pl.when(kc > 0)
                def _():
                    pbuf[...] += product

                @pl.when(kc == n_x1 - 1)
                def _():
                    put = pltpu.make_async_copy(pbuf, stage.at[unit_rows(u), tile_cols(t)], o_sem)
                    put.start()
                    put.wait()
                    part_copy(u, t).start()

                return carry

            lax.fori_loop(0, steps, body, 0)

        pl.run_scoped(
            scope,
            pltpu.VMEM((unit, k_half), jnp.bfloat16),
            pltpu.VMEM((B_BUFFERS, x1_depth, tile), jnp.bfloat16),
            pltpu.VMEM((unit, tile), jnp.float32),
        )

    def finish(units):
        def scope(pbuf, obuf, p_sem, w_sem):
            steps = len(units) * n_tiles

            def place(s):
                u = jnp.int32(units[0])
                for q in range(1, len(units)):
                    u = jnp.where(lax.div(s, n_tiles) == q, jnp.int32(units[q]), u)
                return u, lax.rem(s, n_tiles)

            def start(s):
                u, t = place(s)
                slot = lax.rem(s, 2)
                part_copy(u, t).wait_recv()
                pltpu.make_async_copy(part.at[unit_rows(u), tile_cols(t)], pbuf.at[slot], p_sem.at[slot]).start()

            def put(s):
                u, t = place(s)
                slot = lax.rem(s, 2)
                return pltpu.make_async_copy(obuf.at[slot], out.at[unit_rows(u), tile_cols(t)], w_sem.at[slot])

            start(jnp.int32(0))

            def body(s, carry):
                u, t = place(s)
                slot = lax.rem(s, 2)

                @pl.when(s + 1 < steps)
                def _():
                    start(s + 1)

                @pl.when(s >= 2)
                def _():
                    put(s - 2).wait()

                pltpu.make_async_copy(part.at[unit_rows(u), tile_cols(t)], pbuf.at[slot], p_sem.at[slot]).wait()
                obuf[slot] = (acc[unit_rows(u), tile_cols(t)] + pbuf[slot]).astype(out.dtype)
                put(s).start()
                return carry

            lax.fori_loop(0, steps, body, 0)
            put(jnp.int32(steps - 2)).wait()
            put(jnp.int32(steps - 1)).wait()

        pl.run_scoped(
            scope,
            pltpu.VMEM((2, unit, tile), jnp.float32),
            pltpu.VMEM((2, unit, tile), out.dtype),
            pltpu.SemaphoreType.DMA((2,)),
            pltpu.SemaphoreType.DMA((2,)),
        )

    half = n_x0 // 2
    quarter = n_x0 // 4

    @pl.when(diag)
    def _():
        each(half, lambda c: x0_copy(c).start())
        each(8, lambda c: far_copy(c).start())
        own_rows(0, half, a, b)
        own_rows(half, n_x0, a, b_far, b_ready=lambda c: far_copy(c).wait_recv())
        for u in (0, 1):
            x1_forward(u).wait_recv()
            x1_forward(u).start()
            if u == 1:
                each(half, lambda c: x0_copy(c + half).start())
            other_rows(u)
        for u in (2, 3):
            x1_forward(u).wait_recv()
            other_rows(u)
        finish((2, 3, 0, 1))
        each(n_x0, lambda c: x0_copy(c).wait_send())
        for u in (0, 1):
            x1_forward(u).wait_send()

    @pl.when(off)
    def _():
        for u in (0, 1):
            x1_send(u, vertical).start()
        for u in (2, 3):
            x1_send(u, opposite).start()
        each(8, lambda c: far_copy(c).start())
        arrived = lambda c: x0_copy(c).wait_recv()
        own_rows(0, quarter, x0, b, ready=arrived)
        x1_forward(2).wait_recv()
        x1_forward(2).start()
        each(8, lambda c: far_copy(c).wait_recv())
        other_rows(2)
        own_rows(quarter, half, x0, b, ready=arrived)
        x1_forward(3).wait_recv()
        x1_forward(3).start()
        other_rows(3)
        for u in (0, 1):
            x1_forward(u).wait_recv()
            other_rows(u)
        own_rows(half, n_x0, x0, b_far, ready=arrived)
        finish((0, 1, 2, 3))
        for u in range(UNITS):
            x1_send(u, vertical).wait_send()
        for u in (2, 3):
            x1_forward(u).wait_send()

    each(8, lambda c: far_copy(c).wait_send())
    for u in range(UNITS):
        each(n_tiles, lambda t: part_copy(u, t).wait_send())


def solution(mesh):
    grid_spec = P(("dp", "ri", "ro"), "co")

    def local_block(a_block, b_block):
        rows, k_half = a_block.shape
        k_quarter, cols = b_block.shape
        sizes = make_sizes(rows, k_half, cols)
        n_x0 = k_half // sizes["x0_depth"]
        n_part = UNITS * (cols // sizes["tile"])
        dma = pltpu.SemaphoreType.DMA
        results = pl.pallas_call(
            functools.partial(kernel, sizes),
            out_shape=[
                jax.ShapeDtypeStruct((rows, cols), jnp.bfloat16),
                jax.ShapeDtypeStruct((k_quarter, cols), jnp.bfloat16),
                jax.ShapeDtypeStruct((rows, k_half), jnp.bfloat16),
                jax.ShapeDtypeStruct((rows, k_half), jnp.bfloat16),
                jax.ShapeDtypeStruct((rows, cols), jnp.float32),
                jax.ShapeDtypeStruct((rows, cols), jnp.float32),
            ],
            in_specs=[pl.BlockSpec(memory_space=pl.ANY)] * 2,
            out_specs=[pl.BlockSpec(memory_space=pl.ANY)] * 6,
            scratch_shapes=[
                pltpu.VMEM((rows, cols), jnp.float32),
                dma((8,)),
                dma((8,)),
                dma((n_x0,)),
                dma((n_x0,)),
                dma((UNITS,)),
                dma((UNITS,)),
                dma((UNITS,)),
                dma((n_part,)),
                dma((n_part,)),
                dma((B_BUFFERS,)),
                dma,
                dma,
            ],
            compiler_params=pltpu.CompilerParams(
                collective_id=0, has_side_effects=True, vmem_limit_bytes=63 * 1024 * 1024
            ),
        )(a_block, b_block)
        return results[0]

    return jax.shard_map(local_block, mesh=mesh, in_specs=(grid_spec, grid_spec), out_specs=grid_spec, check_vma=False)
```

```python
import functools

import jax
import jax.numpy as jnp
from jax import lax
from jax.experimental import pallas as pl
from jax.experimental.pallas import tpu as pltpu
from jax.sharding import PartitionSpec as P

MESH = pl.DeviceIdType.MESH
UNITS = 4
B_BUFFERS = 3
P_BUFFERS = 4


def make_sizes(rows, k_half, cols):
    k_quarter = k_half // 2
    return dict(
        rows=rows,
        k_half=k_half,
        k_quarter=k_quarter,
        cols=cols,
        unit=rows // UNITS,
        tile=cols // 8,
        x0_depth=k_quarter // 8,
        tail_depth=max(k_quarter // 32, 128),
        x1_depth=k_quarter // 4,
    )


def kernel(sizes, a, b, acc, b_far, x0, x1, stage, part, far_s, far_r, x0_s, x0_r, tail_s, tail_r, x1_s, x1_r, fwd_s, part_s, part_r, b_sem, x_sem, o_sem):
    rows, k_half, k_quarter = sizes["rows"], sizes["k_half"], sizes["k_quarter"]
    unit, tile = sizes["unit"], sizes["tile"]
    n_tiles = sizes["cols"] // tile
    i, j, r = lax.axis_index("ri"), lax.axis_index("co"), lax.axis_index("ro")
    dp = lax.axis_index("dp")
    vertical, horizontal = (dp, 1 - i, j, r), (dp, i, 1 - j, r)
    opposite, partner = (dp, 1 - i, 1 - j, r), (dp, i, j, 1 - r)
    diag = i == j
    off = jnp.logical_not(diag)

    barrier = pltpu.get_barrier_semaphore()
    for device in (vertical, horizontal, opposite, partner):
        pl.semaphore_signal(barrier, inc=1, device_id=device, device_id_type=MESH)
    pl.semaphore_wait(barrier, 4)

    def remote(src, dst, send, recv, device):
        return pltpu.make_async_remote_copy(
            src_ref=src, dst_ref=dst, send_sem=send, recv_sem=recv, device_id=device, device_id_type=MESH
        )

    far_rows = k_quarter // 8

    def far_copy(c):
        block = pl.ds(c * far_rows, far_rows)
        return remote(b.at[block], b_far.at[block], far_s.at[c], far_r.at[c], partner)

    def k_column(kc, depth):
        return pl.multiple_of(lax.rem(r * k_quarter + kc * depth, k_half), depth)

    x0_depth, tail_depth = sizes["x0_depth"], sizes["tail_depth"]
    n_x0 = k_half // x0_depth
    n_tail = x0_depth // tail_depth

    def x0_copy(kc):
        block = pl.ds(k_column(kc, x0_depth), x0_depth)
        return remote(a.at[:, block], x0.at[:, block], x0_s.at[kc], x0_r.at[kc], horizontal)

    def tail_copy(kc):
        block = pl.ds(k_column(kc, tail_depth), tail_depth)
        q = kc - (n_x0 - 1) * n_tail
        return remote(a.at[:, block], x0.at[:, block], tail_s.at[q], tail_r.at[q], horizontal)

    def unit_rows(u):
        return pl.ds(pl.multiple_of(u * unit, unit), unit)

    def x1_send(u, device):
        return remote(a.at[unit_rows(u)], x1.at[unit_rows(u)], x1_s.at[u], x1_r.at[u], device)

    def x1_forward(u):
        return remote(x1.at[unit_rows(u)], x1.at[unit_rows(u)], fwd_s.at[u], x1_r.at[u], horizontal)

    def tile_cols(t):
        return pl.ds(pl.multiple_of(t * tile, tile), tile)

    def part_copy(u, t):
        where = (unit_rows(u), tile_cols(t))
        return remote(stage.at[where], part.at[where], part_s.at[u * n_tiles + t], part_r.at[u * n_tiles + t], vertical)

    def each(n, step):
        def body(c, carry):
            step(c)
            return carry

        lax.fori_loop(0, n, body, 0)

    def own_rows(first, last, source, b_source, ready=None, b_ready=None, depth=x0_depth):
        far = first * depth >= k_quarter
        base = first - k_quarter // depth if far else first
        steps = (last - first) * n_tiles

        def scope(xbuf, bbuf):
            def b_copy(s):
                c = lax.div(s, n_tiles)
                t = lax.rem(s, n_tiles)
                slot = lax.rem(s, B_BUFFERS)
                k_rows = pl.ds(pl.multiple_of((base + c) * depth, depth), depth)
                return pltpu.make_async_copy(b_source.at[k_rows, tile_cols(t)], bbuf.at[slot], b_sem.at[slot])

            def b_start(s):
                if b_ready is not None:

                    @pl.when(lax.rem(s, n_tiles) == 0)
                    def _():
                        b_ready(base + lax.div(s, n_tiles))

                b_copy(s).start()

            for s in range(B_BUFFERS - 1):
                b_start(jnp.int32(s))

            def body(s, carry):
                c = lax.div(s, n_tiles)
                t = lax.rem(s, n_tiles)

                @pl.when(s + B_BUFFERS - 1 < steps)
                def _():
                    b_start(s + B_BUFFERS - 1)

                @pl.when(t == 0)
                def _():
                    if ready is not None:
                        ready(first + c)
                    block = pl.ds(k_column(first + c, depth), depth)
                    copy = pltpu.make_async_copy(source.at[:, block], xbuf, x_sem)
                    copy.start()
                    copy.wait()

                b_copy(s).wait()
                product = jnp.dot(xbuf[...], bbuf[lax.rem(s, B_BUFFERS)], preferred_element_type=jnp.float32)
                if first == 0:

                    @pl.when(c == 0)
                    def _():
                        acc[:, tile_cols(t)] = product

                    @pl.when(c > 0)
                    def _():
                        acc[:, tile_cols(t)] += product
                else:
                    acc[:, tile_cols(t)] += product
                return carry

            lax.fori_loop(0, steps, body, 0)

        pl.run_scoped(
            scope,
            pltpu.VMEM((rows, depth), jnp.bfloat16),
            pltpu.VMEM((B_BUFFERS, depth, tile), jnp.bfloat16),
        )

    x1_depth = sizes["x1_depth"]
    n_x1 = k_half // x1_depth

    def other_rows(u):
        steps = n_tiles * n_x1

        def scope(xbuf, bbuf, pbuf):
            def b_start(s):
                t = lax.div(s, n_x1)
                kc = lax.rem(s, n_x1)
                slot = lax.rem(s, B_BUFFERS)

                @pl.when(kc < n_x1 // 2)
                def _():
                    k_rows = pl.ds(pl.multiple_of(kc * x1_depth, x1_depth), x1_depth)
                    pltpu.make_async_copy(b.at[k_rows, tile_cols(t)], bbuf.at[slot], b_sem.at[slot]).start()

                @pl.when(kc >= n_x1 // 2)
                def _():
                    k_rows = pl.ds(pl.multiple_of((kc - n_x1 // 2) * x1_depth, x1_depth), x1_depth)
                    pltpu.make_async_copy(b_far.at[k_rows, tile_cols(t)], bbuf.at[slot], b_sem.at[slot]).start()

            load = pltpu.make_async_copy(x1.at[unit_rows(u)], xbuf, x_sem)
            load.start()
            for s in range(B_BUFFERS - 1):
                b_start(jnp.int32(s))
            load.wait()

            def body(s, carry):
                t = lax.div(s, n_x1)
                kc = lax.rem(s, n_x1)
                slot = lax.rem(s, B_BUFFERS)

                @pl.when(s + B_BUFFERS - 1 < steps)
                def _():
                    b_start(s + B_BUFFERS - 1)

                pltpu.make_async_copy(b.at[pl.ds(0, x1_depth), pl.ds(0, tile)], bbuf.at[slot], b_sem.at[slot]).wait()
                columns = pl.ds(k_column(kc, x1_depth), x1_depth)
                product = jnp.dot(xbuf[:, columns], bbuf[slot], preferred_element_type=jnp.float32)

                @pl.when(kc == 0)
                def _():
                    pbuf[...] = product

                @pl.when(kc > 0)
                def _():
                    pbuf[...] += product

                @pl.when(kc == n_x1 - 1)
                def _():
                    put = pltpu.make_async_copy(pbuf, stage.at[unit_rows(u), tile_cols(t)], o_sem)
                    put.start()
                    put.wait()
                    part_copy(u, t).start()

                return carry

            lax.fori_loop(0, steps, body, 0)

        pl.run_scoped(
            scope,
            pltpu.VMEM((unit, k_half), jnp.bfloat16),
            pltpu.VMEM((B_BUFFERS, x1_depth, tile), jnp.bfloat16),
            pltpu.VMEM((unit, tile), jnp.float32),
        )

    def add_parts(first, last):
        depth = min(P_BUFFERS, last - first)

        def scope(pbuf, p_sem):
            def fetch(s):
                where = (unit_rows(lax.div(s, n_tiles)), tile_cols(lax.rem(s, n_tiles)))
                slot = lax.rem(s, P_BUFFERS)
                return pltpu.make_async_copy(part.at[where], pbuf.at[slot], p_sem.at[slot])

            def start(s):
                part_copy(lax.div(s, n_tiles), lax.rem(s, n_tiles)).wait_recv()
                fetch(s).start()

            for s in range(first, first + depth - 1):
                start(jnp.int32(s))

            def body(s, carry):
                @pl.when(s + depth - 1 < last)
                def _():
                    start(s + depth - 1)

                fetch(s).wait()
                acc[unit_rows(lax.div(s, n_tiles)), tile_cols(lax.rem(s, n_tiles))] += pbuf[lax.rem(s, P_BUFFERS)]
                return carry

            lax.fori_loop(first, last, body, 0)

        pl.run_scoped(
            scope,
            pltpu.VMEM((P_BUFFERS, unit, tile), jnp.float32),
            pltpu.SemaphoreType.DMA((P_BUFFERS,)),
        )

    half = n_x0 // 2
    quarter = n_x0 // 4
    last = n_x0 - 1
    tail = (last * n_tail, n_x0 * n_tail)

    @pl.when(diag)
    def _():
        each(half, lambda c: x0_copy(c).start())
        each(8, lambda c: far_copy(c).start())
        own_rows(0, half, a, b)
        own_rows(half, n_x0 - 2, a, b_far, b_ready=lambda c: far_copy(c).wait_recv())
        for c in (6, 7):
            far_copy(c).wait_recv()
        x1_forward(0).wait_recv()
        x1_forward(0).start()
        other_rows(0)
        x1_forward(1).wait_recv()
        x1_forward(1).start()
        each(half - 1, lambda c: x0_copy(c + half).start())
        each(n_tail, lambda c: tail_copy(tail[0] + c).start())
        own_rows(n_x0 - 2, n_x0, a, b_far)
        for u in (1, 2, 3):
            if u > 1:
                x1_forward(u).wait_recv()
            other_rows(u)
        add_parts(2 * n_tiles, 4 * n_tiles)
        add_parts(0, 2 * n_tiles)
        each(last, lambda c: x0_copy(c).wait_send())
        each(n_tail, lambda c: tail_copy(tail[0] + c).wait_send())
        for u in (0, 1):
            x1_forward(u).wait_send()

    @pl.when(off)
    def _():
        for u in (0, 1):
            x1_send(u, vertical).start()
        for u in (2, 3):
            x1_send(u, opposite).start()
        each(8, lambda c: far_copy(c).start())
        arrived = lambda c: x0_copy(c).wait_recv()
        own_rows(0, quarter, x0, b, ready=arrived)
        x1_forward(2).wait_recv()
        x1_forward(2).start()
        each(8, lambda c: far_copy(c).wait_recv())
        other_rows(2)
        own_rows(quarter, half, x0, b, ready=arrived)
        x1_forward(3).wait_recv()
        x1_forward(3).start()
        other_rows(3)
        for u in (0, 1):
            x1_forward(u).wait_recv()
            other_rows(u)
        own_rows(half, half + 4, x0, b_far, ready=arrived)
        add_parts(0, 2 * n_tiles)
        own_rows(half + 4, last - 1, x0, b_far, ready=arrived)
        add_parts(2 * n_tiles, 3 * n_tiles)
        own_rows(last - 1, last, x0, b_far, ready=arrived)
        add_parts(3 * n_tiles, 3 * n_tiles + 6)
        own_rows(*tail, x0, b_far, ready=lambda c: tail_copy(c).wait_recv(), depth=tail_depth)
        add_parts(3 * n_tiles + 6, 4 * n_tiles)
        for u in range(UNITS):
            x1_send(u, vertical).wait_send()
        for u in (2, 3):
            x1_forward(u).wait_send()

    each(8, lambda c: far_copy(c).wait_send())
    for u in range(UNITS):
        each(n_tiles, lambda t: part_copy(u, t).wait_send())


def solution(mesh):
    grid_spec = P(("dp", "ri", "ro"), "co")

    def local_block(a_block, b_block):
        rows, k_half = a_block.shape
        k_quarter, cols = b_block.shape
        sizes = make_sizes(rows, k_half, cols)
        n_x0 = k_half // sizes["x0_depth"]
        n_tail = sizes["x0_depth"] // sizes["tail_depth"]
        n_part = UNITS * (cols // sizes["tile"])
        dma = pltpu.SemaphoreType.DMA
        results = pl.pallas_call(
            functools.partial(kernel, sizes),
            out_shape=[
                pltpu.VMEM((rows, cols), jnp.float32),
                jax.ShapeDtypeStruct((k_quarter, cols), jnp.bfloat16),
                jax.ShapeDtypeStruct((rows, k_half), jnp.bfloat16),
                jax.ShapeDtypeStruct((rows, k_half), jnp.bfloat16),
                jax.ShapeDtypeStruct((rows, cols), jnp.float32),
                jax.ShapeDtypeStruct((rows, cols), jnp.float32),
            ],
            in_specs=[pl.BlockSpec(memory_space=pl.ANY)] * 2,
            out_specs=[pl.BlockSpec(memory_space=pltpu.VMEM)] + [pl.BlockSpec(memory_space=pl.ANY)] * 5,
            scratch_shapes=[
                dma((8,)),
                dma((8,)),
                dma((n_x0,)),
                dma((n_x0,)),
                dma((n_tail,)),
                dma((n_tail,)),
                dma((UNITS,)),
                dma((UNITS,)),
                dma((UNITS,)),
                dma((n_part,)),
                dma((n_part,)),
                dma((B_BUFFERS,)),
                dma,
                dma,
            ],
            compiler_params=pltpu.CompilerParams(
                collective_id=0, has_side_effects=True, vmem_limit_bytes=30 * 1024 * 1024
            ),
        )(a_block, b_block)
        return results[0].astype(jnp.bfloat16)

    return jax.shard_map(local_block, mesh=mesh, in_specs=(grid_spec, grid_spec), out_specs=grid_spec, check_vma=False)
```

```python
import functools

import jax
import jax.numpy as jnp
from jax import lax
from jax.experimental import pallas as pl
from jax.experimental.pallas import tpu as pltpu
from jax.sharding import PartitionSpec as P

MESH = pl.DeviceIdType.MESH
UNITS = 4
B_BUFFERS = 3
P_BUFFERS = 4


def make_sizes(rows, k_half, cols):
    k_quarter = k_half // 2
    return dict(
        rows=rows,
        k_half=k_half,
        k_quarter=k_quarter,
        cols=cols,
        unit=rows // UNITS,
        tile=cols // 8,
        x0_depth=k_quarter // 8,
        tail_depth=k_quarter // 16,
        x1_depth=k_quarter // 4,
    )


def kernel(sizes, a, b, acc, b_far, x0, x1, stage, part, far_s, far_r, x_last, part_last, x0_s, x0_r, tail_s, tail_r, last_s, last_r, x1_s, x1_r, fwd_s, part_s, part_r, end_s, end_r, b_sem, x_sem, o_sem):
    rows, k_half, k_quarter = sizes["rows"], sizes["k_half"], sizes["k_quarter"]
    unit, tile = sizes["unit"], sizes["tile"]
    n_tiles = sizes["cols"] // tile
    i, j, r = lax.axis_index("ri"), lax.axis_index("co"), lax.axis_index("ro")
    dp = lax.axis_index("dp")
    vertical, horizontal = (dp, 1 - i, j, r), (dp, i, 1 - j, r)
    opposite, partner = (dp, 1 - i, 1 - j, r), (dp, i, j, 1 - r)
    diag = i == j
    off = jnp.logical_not(diag)

    barrier = pltpu.get_barrier_semaphore()
    for device in (vertical, horizontal, opposite, partner):
        pl.semaphore_signal(barrier, inc=1, device_id=device, device_id_type=MESH)
    pl.semaphore_wait(barrier, 4)

    def remote(src, dst, send, recv, device):
        return pltpu.make_async_remote_copy(
            src_ref=src, dst_ref=dst, send_sem=send, recv_sem=recv, device_id=device, device_id_type=MESH
        )

    far_rows = k_quarter // 8

    def far_copy(c):
        block = pl.ds(c * far_rows, far_rows)
        return remote(b.at[block], b_far.at[block], far_s.at[c], far_r.at[c], partner)

    def k_column(kc, depth):
        return pl.multiple_of(lax.rem(r * k_quarter + kc * depth, k_half), depth)

    def unit_rows(u):
        return pl.ds(pl.multiple_of(u * unit, unit), unit)

    x0_depth, tail_depth = sizes["x0_depth"], sizes["tail_depth"]
    n_x0 = k_half // x0_depth
    n_tail = k_half // tail_depth

    def x0_copy(kc):
        block = pl.ds(k_column(kc, x0_depth), x0_depth)
        return remote(a.at[:, block], x0.at[:, block], x0_s.at[kc], x0_r.at[kc], horizontal)

    def tail_copy(kc):
        block = pl.ds(k_column(kc, tail_depth), tail_depth)
        q = kc - n_tail // 2
        return remote(a.at[:, block], x0.at[:, block], tail_s.at[q], tail_r.at[q], horizontal)

    def last_copy(q):
        block = pl.ds(k_column(n_tail - 1, tail_depth), tail_depth)
        return remote(a.at[unit_rows(q), block], x_last.at[unit_rows(q)], last_s.at[q], last_r.at[q], horizontal)

    def x1_send(u, device):
        return remote(a.at[unit_rows(u)], x1.at[unit_rows(u)], x1_s.at[u], x1_r.at[u], device)

    def x1_forward(u):
        return remote(x1.at[unit_rows(u)], x1.at[unit_rows(u)], fwd_s.at[u], x1_r.at[u], horizontal)

    def tile_cols(t):
        return pl.ds(pl.multiple_of(t * tile, tile), tile)

    def part_copy(u, t):
        where = (unit_rows(u), tile_cols(t))
        return remote(stage.at[where], part.at[where], part_s.at[u * n_tiles + t], part_r.at[u * n_tiles + t], vertical)

    def end_copy(u):
        return remote(stage.at[unit_rows(u), tile_cols(n_tiles - 1)], part_last, end_s, end_r, vertical)

    def each(n, step):
        def body(c, carry):
            step(c)
            return carry

        lax.fori_loop(0, n, body, 0)

    def own_rows(first, last, source, b_source, ready=None, b_ready=None, depth=x0_depth):
        far = first * depth >= k_quarter
        base = first - k_quarter // depth if far else first
        steps = (last - first) * n_tiles

        def scope(xbuf, bbuf):
            def b_copy(s):
                c = lax.div(s, n_tiles)
                t = lax.rem(s, n_tiles)
                slot = lax.rem(s, B_BUFFERS)
                k_rows = pl.ds(pl.multiple_of((base + c) * depth, depth), depth)
                return pltpu.make_async_copy(b_source.at[k_rows, tile_cols(t)], bbuf.at[slot], b_sem.at[slot])

            def b_start(s):
                if b_ready is not None:

                    @pl.when(lax.rem(s, n_tiles) == 0)
                    def _():
                        b_ready(base + lax.div(s, n_tiles))

                b_copy(s).start()

            for s in range(B_BUFFERS - 1):
                b_start(jnp.int32(s))

            def body(s, carry):
                c = lax.div(s, n_tiles)
                t = lax.rem(s, n_tiles)

                @pl.when(s + B_BUFFERS - 1 < steps)
                def _():
                    b_start(s + B_BUFFERS - 1)

                @pl.when(t == 0)
                def _():
                    if ready is not None:
                        ready(first + c)
                    block = pl.ds(k_column(first + c, depth), depth)
                    copy = pltpu.make_async_copy(source.at[:, block], xbuf, x_sem)
                    copy.start()
                    copy.wait()

                b_copy(s).wait()
                product = jnp.dot(xbuf[...], bbuf[lax.rem(s, B_BUFFERS)], preferred_element_type=jnp.float32)
                if first == 0:

                    @pl.when(c == 0)
                    def _():
                        acc[:, tile_cols(t)] = product

                    @pl.when(c > 0)
                    def _():
                        acc[:, tile_cols(t)] += product
                else:
                    acc[:, tile_cols(t)] += product
                return carry

            lax.fori_loop(0, steps, body, 0)

        pl.run_scoped(
            scope,
            pltpu.VMEM((rows, depth), jnp.bfloat16),
            pltpu.VMEM((B_BUFFERS, depth, tile), jnp.bfloat16),
        )

    x1_depth = sizes["x1_depth"]
    n_x1 = k_half // x1_depth

    def other_rows(u, final=False):
        steps = n_tiles * n_x1

        def scope(xbuf, bbuf, pbuf):
            def b_start(s):
                t = lax.div(s, n_x1)
                kc = lax.rem(s, n_x1)
                slot = lax.rem(s, B_BUFFERS)

                @pl.when(kc < n_x1 // 2)
                def _():
                    k_rows = pl.ds(pl.multiple_of(kc * x1_depth, x1_depth), x1_depth)
                    pltpu.make_async_copy(b.at[k_rows, tile_cols(t)], bbuf.at[slot], b_sem.at[slot]).start()

                @pl.when(kc >= n_x1 // 2)
                def _():
                    k_rows = pl.ds(pl.multiple_of((kc - n_x1 // 2) * x1_depth, x1_depth), x1_depth)
                    pltpu.make_async_copy(b_far.at[k_rows, tile_cols(t)], bbuf.at[slot], b_sem.at[slot]).start()

            load = pltpu.make_async_copy(x1.at[unit_rows(u)], xbuf, x_sem)
            load.start()
            for s in range(B_BUFFERS - 1):
                b_start(jnp.int32(s))
            load.wait()

            def body(s, carry):
                t = lax.div(s, n_x1)
                kc = lax.rem(s, n_x1)
                slot = lax.rem(s, B_BUFFERS)

                @pl.when(s + B_BUFFERS - 1 < steps)
                def _():
                    b_start(s + B_BUFFERS - 1)

                pltpu.make_async_copy(b.at[pl.ds(0, x1_depth), pl.ds(0, tile)], bbuf.at[slot], b_sem.at[slot]).wait()
                columns = pl.ds(k_column(kc, x1_depth), x1_depth)
                product = jnp.dot(xbuf[:, columns], bbuf[slot], preferred_element_type=jnp.float32)

                @pl.when(kc == 0)
                def _():
                    pbuf[...] = product

                @pl.when(kc > 0)
                def _():
                    pbuf[...] += product

                @pl.when(kc == n_x1 - 1)
                def _():
                    put = pltpu.make_async_copy(pbuf, stage.at[unit_rows(u), tile_cols(t)], o_sem)
                    put.start()
                    put.wait()
                    if final:

                        @pl.when(t < n_tiles - 1)
                        def _():
                            part_copy(u, t).start()

                        @pl.when(t == n_tiles - 1)
                        def _():
                            end_copy(u).start()
                    else:
                        part_copy(u, t).start()

                return carry

            lax.fori_loop(0, steps, body, 0)

        pl.run_scoped(
            scope,
            pltpu.VMEM((unit, k_half), jnp.bfloat16),
            pltpu.VMEM((B_BUFFERS, x1_depth, tile), jnp.bfloat16),
            pltpu.VMEM((unit, tile), jnp.float32),
        )

    def add_parts(first, last, depth=P_BUFFERS):
        depth = min(depth, last - first)

        def scope(pbuf, p_sem):
            def fetch(s):
                where = (unit_rows(lax.div(s, n_tiles)), tile_cols(lax.rem(s, n_tiles)))
                slot = lax.rem(s, P_BUFFERS)
                return pltpu.make_async_copy(part.at[where], pbuf.at[slot], p_sem.at[slot])

            def start(s):
                part_copy(lax.div(s, n_tiles), lax.rem(s, n_tiles)).wait_recv()
                fetch(s).start()

            for s in range(first, first + depth - 1):
                start(jnp.int32(s))

            def body(s, carry):
                @pl.when(s + depth - 1 < last)
                def _():
                    start(s + depth - 1)

                fetch(s).wait()
                acc[unit_rows(lax.div(s, n_tiles)), tile_cols(lax.rem(s, n_tiles))] += pbuf[lax.rem(s, P_BUFFERS)]
                return carry

            lax.fori_loop(first, last, body, 0)

        pl.run_scoped(
            scope,
            pltpu.VMEM((P_BUFFERS, unit, tile), jnp.float32),
            pltpu.SemaphoreType.DMA((P_BUFFERS,)),
        )

    def add_end(u):
        end_copy(u).wait_recv()
        acc[unit_rows(u), tile_cols(n_tiles - 1)] += part_last[...]

    def last_rows(before, between):
        def scope(bbuf):
            load = pltpu.make_async_copy(b_far.at[pl.ds(k_quarter - tail_depth, tail_depth)], bbuf, o_sem)
            load.start()
            before()
            load.wait()

            def step(q):
                last_copy(q).wait_recv()
                for t in range(n_tiles):
                    columns = pl.ds(t * tile, tile)
                    acc[unit_rows(q), columns] += jnp.dot(
                        x_last[unit_rows(q), :], bbuf[:, columns], preferred_element_type=jnp.float32
                    )

            each(UNITS - 1, step)
            between()
            each(1, lambda q: step(q + UNITS - 1))

        pl.run_scoped(scope, pltpu.VMEM((tail_depth, sizes["cols"]), jnp.bfloat16))

    half = n_x0 // 2
    quarter = n_x0 // 4
    thin = n_tail // 2

    @pl.when(diag)
    def _():
        each(half, lambda c: x0_copy(c).start())
        each(8, lambda c: far_copy(c).start())
        own_rows(0, half, a, b)
        own_rows(half, n_x0 - 2, a, b_far, b_ready=lambda c: far_copy(c).wait_recv())
        for c in (6, 7):
            far_copy(c).wait_recv()
        x1_forward(0).wait_recv()
        x1_forward(0).start()
        other_rows(0)
        x1_forward(1).wait_recv()
        x1_forward(1).start()
        each(thin - 1, lambda c: tail_copy(thin + c).start())
        each(UNITS, lambda q: last_copy(q).start())
        own_rows(n_x0 - 2, n_x0, a, b_far)
        other_rows(1)
        for u in (2, 3):
            x1_forward(u).wait_recv()
            other_rows(u, final=u == 3)
        add_parts(2 * n_tiles, 4 * n_tiles)
        add_parts(0, n_tiles)
        add_parts(n_tiles, 2 * n_tiles - 1, depth=1)
        add_end(1)
        each(half, lambda c: x0_copy(c).wait_send())
        each(thin - 1, lambda c: tail_copy(thin + c).wait_send())
        each(UNITS, lambda q: last_copy(q).wait_send())
        for u in (0, 1):
            x1_forward(u).wait_send()
        for u in (0, 1, 2):
            each(n_tiles, lambda t: part_copy(u, t).wait_send())
        each(n_tiles - 1, lambda t: part_copy(3, t).wait_send())
        end_copy(3).wait_send()

    @pl.when(off)
    def _():
        for u in (0, 1):
            x1_send(u, vertical).start()
        for u in (2, 3):
            x1_send(u, opposite).start()
        each(8, lambda c: far_copy(c).start())
        arrived = lambda c: x0_copy(c).wait_recv()
        own_rows(0, quarter, x0, b, ready=arrived)
        x1_forward(2).wait_recv()
        x1_forward(2).start()
        each(8, lambda c: far_copy(c).wait_recv())
        other_rows(2)
        own_rows(quarter, half, x0, b, ready=arrived)
        x1_forward(3).wait_recv()
        x1_forward(3).start()
        other_rows(3)
        for u in (0, 1):
            x1_forward(u).wait_recv()
            other_rows(u, final=u == 1)
        thin_arrived = lambda c: tail_copy(c).wait_recv()
        rest = lambda first, last: own_rows(first, last, x0, b_far, ready=thin_arrived, depth=tail_depth)
        rest(thin, thin + 8)
        add_parts(0, 2 * n_tiles)
        rest(thin + 8, n_tail - 4)
        add_parts(2 * n_tiles, 3 * n_tiles + 4)
        rest(n_tail - 4, n_tail - 2)
        add_parts(3 * n_tiles + 4, 3 * n_tiles + 6)
        last_rows(
            before=lambda: rest(n_tail - 2, n_tail - 1),
            between=lambda: add_parts(3 * n_tiles + 6, 4 * n_tiles - 1),
        )
        add_end(3)
        for u in range(UNITS):
            x1_send(u, vertical).wait_send()
        for u in (2, 3):
            x1_forward(u).wait_send()
        for u in (0, 2, 3):
            each(n_tiles, lambda t: part_copy(u, t).wait_send())
        each(n_tiles - 1, lambda t: part_copy(1, t).wait_send())
        end_copy(1).wait_send()

    each(8, lambda c: far_copy(c).wait_send())


def solution(mesh):
    grid_spec = P(("dp", "ri", "ro"), "co")

    def local_block(a_block, b_block):
        rows, k_half = a_block.shape
        k_quarter, cols = b_block.shape
        sizes = make_sizes(rows, k_half, cols)
        n_x0 = k_half // sizes["x0_depth"]
        n_tail = k_half // sizes["tail_depth"]
        n_part = UNITS * (cols // sizes["tile"])
        dma = pltpu.SemaphoreType.DMA
        results = pl.pallas_call(
            functools.partial(kernel, sizes),
            out_shape=[
                pltpu.VMEM((rows, cols), jnp.float32),
                jax.ShapeDtypeStruct((k_quarter, cols), jnp.bfloat16),
                jax.ShapeDtypeStruct((rows, k_half), jnp.bfloat16),
                jax.ShapeDtypeStruct((rows, k_half), jnp.bfloat16),
                jax.ShapeDtypeStruct((rows, cols), jnp.float32),
                jax.ShapeDtypeStruct((rows, cols), jnp.float32),
            ],
            in_specs=[pl.BlockSpec(memory_space=pl.ANY)] * 2,
            out_specs=[pl.BlockSpec(memory_space=pltpu.VMEM)] + [pl.BlockSpec(memory_space=pl.ANY)] * 5,
            scratch_shapes=[
                dma((8,)),
                dma((8,)),
                pltpu.VMEM((rows, sizes["tail_depth"]), jnp.bfloat16),
                pltpu.VMEM((sizes["unit"], sizes["tile"]), jnp.float32),
                dma((n_x0 // 2,)),
                dma((n_x0 // 2,)),
                dma((n_tail // 2 - 1,)),
                dma((n_tail // 2 - 1,)),
                dma((UNITS,)),
                dma((UNITS,)),
                dma((UNITS,)),
                dma((UNITS,)),
                dma((UNITS,)),
                dma((n_part,)),
                dma((n_part,)),
                dma,
                dma,
                dma((B_BUFFERS,)),
                dma,
                dma,
            ],
            compiler_params=pltpu.CompilerParams(
                collective_id=0, has_side_effects=True, vmem_limit_bytes=30 * 1024 * 1024
            ),
        )(a_block, b_block)
        return results[0].astype(jnp.bfloat16)

    return jax.shard_map(local_block, mesh=mesh, in_specs=(grid_spec, grid_spec), out_specs=grid_spec, check_vma=False)
```

```python
import functools

import jax
import jax.numpy as jnp
from jax import lax
from jax.experimental import pallas as pl
from jax.experimental.pallas import tpu as pltpu
from jax.sharding import PartitionSpec as P

MESH = pl.DeviceIdType.MESH
UNITS = 4
B_BUFFERS = 3
P_BUFFERS = 4
R_BUFFERS = 8
R_ROWS = 32


def make_sizes(rows, k_half, cols):
    k_quarter = k_half // 2
    return dict(
        rows=rows,
        k_half=k_half,
        k_quarter=k_quarter,
        cols=cols,
        unit=rows // UNITS,
        tile=cols // 8,
        x0_depth=k_quarter // 8,
        tail_depth=k_quarter // 16,
        x1_depth=k_quarter // 4,
    )


def kernel(sizes, a, b, acc, b_far, x0, x1, stage, part, far_s, far_r, x_last, part_last, x0_s, x0_r, tail_s, tail_r, last_s, last_r, x1_s, x1_r, fwd_s, part_s, part_r, end_s, end_r, b_sem, x_sem, o_sem):
    rows, k_half, k_quarter = sizes["rows"], sizes["k_half"], sizes["k_quarter"]
    unit, tile = sizes["unit"], sizes["tile"]
    n_tiles = sizes["cols"] // tile
    i, j, r = lax.axis_index("ri"), lax.axis_index("co"), lax.axis_index("ro")
    dp = lax.axis_index("dp")
    vertical, horizontal = (dp, 1 - i, j, r), (dp, i, 1 - j, r)
    opposite, partner = (dp, 1 - i, 1 - j, r), (dp, i, j, 1 - r)
    diag = i == j
    off = jnp.logical_not(diag)

    barrier = pltpu.get_barrier_semaphore()
    for device in (vertical, horizontal, opposite, partner):
        pl.semaphore_signal(barrier, inc=1, device_id=device, device_id_type=MESH)
    pl.semaphore_wait(barrier, 4)

    def remote(src, dst, send, recv, device):
        return pltpu.make_async_remote_copy(
            src_ref=src, dst_ref=dst, send_sem=send, recv_sem=recv, device_id=device, device_id_type=MESH
        )

    far_rows = k_quarter // 8

    def far_copy(c):
        block = pl.ds(c * far_rows, far_rows)
        return remote(b.at[block], b_far.at[block], far_s.at[c], far_r.at[c], partner)

    def k_column(kc, depth):
        return pl.multiple_of(lax.rem(r * k_quarter + kc * depth, k_half), depth)

    def unit_rows(u):
        return pl.ds(pl.multiple_of(u * unit, unit), unit)

    x0_depth, tail_depth = sizes["x0_depth"], sizes["tail_depth"]
    n_x0 = k_half // x0_depth
    n_tail = k_half // tail_depth

    def x0_copy(kc):
        block = pl.ds(k_column(kc, x0_depth), x0_depth)
        return remote(a.at[:, block], x0.at[:, block], x0_s.at[kc], x0_r.at[kc], horizontal)

    def tail_copy(kc):
        block = pl.ds(k_column(kc, tail_depth), tail_depth)
        q = kc - n_tail // 2
        return remote(a.at[:, block], x0.at[:, block], tail_s.at[q], tail_r.at[q], horizontal)

    def last_copy(q):
        block = pl.ds(k_column(n_tail - 1, tail_depth), tail_depth)
        return remote(a.at[unit_rows(q), block], x_last.at[unit_rows(q)], last_s.at[q], last_r.at[q], horizontal)

    def x1_send(u, device):
        return remote(a.at[unit_rows(u)], x1.at[unit_rows(u)], x1_s.at[u], x1_r.at[u], device)

    def x1_forward(u):
        return remote(x1.at[unit_rows(u)], x1.at[unit_rows(u)], fwd_s.at[u], x1_r.at[u], horizontal)

    def tile_cols(t):
        return pl.ds(pl.multiple_of(t * tile, tile), tile)

    def part_copy(u, t):
        where = (unit_rows(u), tile_cols(t))
        return remote(stage.at[where], part.at[where], part_s.at[u * n_tiles + t], part_r.at[u * n_tiles + t], vertical)

    def end_copy(u):
        return remote(stage.at[unit_rows(u), tile_cols(n_tiles - 1)], part_last, end_s, end_r, vertical)

    def each(n, step):
        def body(c, carry):
            step(c)
            return carry

        lax.fori_loop(0, n, body, 0)

    def own_rows(first, last, source, b_source, ready=None, b_ready=None, depth=x0_depth):
        far = first * depth >= k_quarter
        base = first - k_quarter // depth if far else first
        steps = (last - first) * n_tiles

        def scope(xbuf, bbuf):
            def b_copy(s):
                c = lax.div(s, n_tiles)
                t = lax.rem(s, n_tiles)
                slot = lax.rem(s, B_BUFFERS)
                k_rows = pl.ds(pl.multiple_of((base + c) * depth, depth), depth)
                return pltpu.make_async_copy(b_source.at[k_rows, tile_cols(t)], bbuf.at[slot], b_sem.at[slot])

            def b_start(s):
                if b_ready is not None:

                    @pl.when(lax.rem(s, n_tiles) == 0)
                    def _():
                        b_ready(base + lax.div(s, n_tiles))

                b_copy(s).start()

            for s in range(B_BUFFERS - 1):
                b_start(jnp.int32(s))

            def body(s, carry):
                c = lax.div(s, n_tiles)
                t = lax.rem(s, n_tiles)

                @pl.when(s + B_BUFFERS - 1 < steps)
                def _():
                    b_start(s + B_BUFFERS - 1)

                @pl.when(t == 0)
                def _():
                    if ready is not None:
                        ready(first + c)
                    block = pl.ds(k_column(first + c, depth), depth)
                    copy = pltpu.make_async_copy(source.at[:, block], xbuf, x_sem)
                    copy.start()
                    copy.wait()

                b_copy(s).wait()
                product = jnp.dot(xbuf[...], bbuf[lax.rem(s, B_BUFFERS)], preferred_element_type=jnp.float32)
                if first == 0:

                    @pl.when(c == 0)
                    def _():
                        acc[:, tile_cols(t)] = product

                    @pl.when(c > 0)
                    def _():
                        acc[:, tile_cols(t)] += product
                else:
                    acc[:, tile_cols(t)] += product
                return carry

            lax.fori_loop(0, steps, body, 0)

        pl.run_scoped(
            scope,
            pltpu.VMEM((rows, depth), jnp.bfloat16),
            pltpu.VMEM((B_BUFFERS, depth, tile), jnp.bfloat16),
        )

    x1_depth = sizes["x1_depth"]
    n_x1 = k_half // x1_depth

    def other_rows(u, final=False):
        steps = n_tiles * n_x1

        def scope(xbuf, bbuf, pbuf):
            def b_start(s):
                t = lax.div(s, n_x1)
                kc = lax.rem(s, n_x1)
                slot = lax.rem(s, B_BUFFERS)

                @pl.when(kc < n_x1 // 2)
                def _():
                    k_rows = pl.ds(pl.multiple_of(kc * x1_depth, x1_depth), x1_depth)
                    pltpu.make_async_copy(b.at[k_rows, tile_cols(t)], bbuf.at[slot], b_sem.at[slot]).start()

                @pl.when(kc >= n_x1 // 2)
                def _():
                    k_rows = pl.ds(pl.multiple_of((kc - n_x1 // 2) * x1_depth, x1_depth), x1_depth)
                    pltpu.make_async_copy(b_far.at[k_rows, tile_cols(t)], bbuf.at[slot], b_sem.at[slot]).start()

            load = pltpu.make_async_copy(x1.at[unit_rows(u)], xbuf, x_sem)
            load.start()
            for s in range(B_BUFFERS - 1):
                b_start(jnp.int32(s))
            load.wait()

            def body(s, carry):
                t = lax.div(s, n_x1)
                kc = lax.rem(s, n_x1)
                slot = lax.rem(s, B_BUFFERS)

                @pl.when(s + B_BUFFERS - 1 < steps)
                def _():
                    b_start(s + B_BUFFERS - 1)

                pltpu.make_async_copy(b.at[pl.ds(0, x1_depth), pl.ds(0, tile)], bbuf.at[slot], b_sem.at[slot]).wait()
                columns = pl.ds(k_column(kc, x1_depth), x1_depth)
                product = jnp.dot(xbuf[:, columns], bbuf[slot], preferred_element_type=jnp.float32)

                @pl.when(kc == 0)
                def _():
                    pbuf[...] = product

                @pl.when(kc > 0)
                def _():
                    pbuf[...] += product

                @pl.when(kc == n_x1 - 1)
                def _():
                    put = pltpu.make_async_copy(pbuf, stage.at[unit_rows(u), tile_cols(t)], o_sem)
                    put.start()
                    put.wait()
                    if final:

                        @pl.when(t < n_tiles - 1)
                        def _():
                            part_copy(u, t).start()

                        @pl.when(t == n_tiles - 1)
                        def _():
                            end_copy(u).start()
                    else:
                        part_copy(u, t).start()

                return carry

            lax.fori_loop(0, steps, body, 0)

        pl.run_scoped(
            scope,
            pltpu.VMEM((unit, k_half), jnp.bfloat16),
            pltpu.VMEM((B_BUFFERS, x1_depth, tile), jnp.bfloat16),
            pltpu.VMEM((unit, tile), jnp.float32),
        )

    def add_parts(first, last, depth=P_BUFFERS):
        depth = min(depth, last - first)

        def scope(pbuf, p_sem):
            def fetch(s):
                where = (unit_rows(lax.div(s, n_tiles)), tile_cols(lax.rem(s, n_tiles)))
                slot = lax.rem(s, P_BUFFERS)
                return pltpu.make_async_copy(part.at[where], pbuf.at[slot], p_sem.at[slot])

            def start(s):
                part_copy(lax.div(s, n_tiles), lax.rem(s, n_tiles)).wait_recv()
                fetch(s).start()

            for s in range(first, first + depth - 1):
                start(jnp.int32(s))

            def body(s, carry):
                @pl.when(s + depth - 1 < last)
                def _():
                    start(s + depth - 1)

                fetch(s).wait()
                acc[unit_rows(lax.div(s, n_tiles)), tile_cols(lax.rem(s, n_tiles))] += pbuf[lax.rem(s, P_BUFFERS)]
                return carry

            lax.fori_loop(first, last, body, 0)

        pl.run_scoped(
            scope,
            pltpu.VMEM((P_BUFFERS, unit, tile), jnp.float32),
            pltpu.SemaphoreType.DMA((P_BUFFERS,)),
        )

    def add_end(u):
        end_copy(u).wait_recv()
        acc[unit_rows(u), tile_cols(n_tiles - 1)] += part_last[...]

    def last_rows(before, between):
        def scope(bbuf):
            load = pltpu.make_async_copy(b_far.at[pl.ds(k_quarter - tail_depth, tail_depth)], bbuf, o_sem)
            load.start()
            before()
            load.wait()

            def step(q):
                last_copy(q).wait_recv()
                for t in range(n_tiles):
                    columns = pl.ds(t * tile, tile)
                    acc[unit_rows(q), columns] += jnp.dot(
                        x_last[unit_rows(q), :], bbuf[:, columns], preferred_element_type=jnp.float32
                    )

            each(UNITS - 1, step)
            between()
            each(1, lambda q: step(q + UNITS - 1))

        pl.run_scoped(scope, pltpu.VMEM((tail_depth, sizes["cols"]), jnp.bfloat16))

    half = n_x0 // 2
    quarter = n_x0 // 4
    thin = n_tail // 2

    @pl.when(diag)
    def _():
        each(half, lambda c: x0_copy(c).start())
        each(8, lambda c: far_copy(c).start())
        own_rows(0, half, a, b)
        own_rows(half, n_x0 - 2, a, b_far, b_ready=lambda c: far_copy(c).wait_recv())
        for c in (6, 7):
            far_copy(c).wait_recv()
        x1_forward(0).wait_recv()
        x1_forward(0).start()
        other_rows(0)
        x1_forward(1).wait_recv()
        x1_forward(1).start()
        each(thin - 1, lambda c: tail_copy(thin + c).start())
        each(UNITS, lambda q: last_copy(q).start())
        own_rows(n_x0 - 2, n_x0, a, b_far)
        other_rows(1)
        for u in (2, 3):
            x1_forward(u).wait_recv()
            other_rows(u, final=u == 3)
        add_parts(2 * n_tiles, 4 * n_tiles)
        add_parts(0, n_tiles)
        add_parts(n_tiles, 2 * n_tiles - 1, depth=1)
        add_end(1)
        each(half, lambda c: x0_copy(c).wait_send())
        each(thin - 1, lambda c: tail_copy(thin + c).wait_send())
        each(UNITS, lambda q: last_copy(q).wait_send())
        for u in (0, 1):
            x1_forward(u).wait_send()
        for u in (0, 1, 2):
            each(n_tiles, lambda t: part_copy(u, t).wait_send())
        each(n_tiles - 1, lambda t: part_copy(3, t).wait_send())
        end_copy(3).wait_send()

    @pl.when(off)
    def _():
        for u in (0, 1):
            x1_send(u, vertical).start()
        for u in (2, 3):
            x1_send(u, opposite).start()
        each(8, lambda c: far_copy(c).start())
        arrived = lambda c: x0_copy(c).wait_recv()
        own_rows(0, quarter, x0, b, ready=arrived)
        x1_forward(2).wait_recv()
        x1_forward(2).start()
        each(8, lambda c: far_copy(c).wait_recv())
        other_rows(2)
        own_rows(quarter, half, x0, b, ready=arrived)
        x1_forward(3).wait_recv()
        x1_forward(3).start()
        other_rows(3)
        for u in (0, 1):
            x1_forward(u).wait_recv()
            other_rows(u, final=u == 1)
        thin_arrived = lambda c: tail_copy(c).wait_recv()
        rest = lambda first, last: own_rows(first, last, x0, b_far, ready=thin_arrived, depth=tail_depth)
        rest(thin, thin + 8)
        add_parts(0, 2 * n_tiles)
        rest(thin + 8, n_tail - 4)
        add_parts(2 * n_tiles, 3 * n_tiles + 4)
        rest(n_tail - 4, n_tail - 2)
        add_parts(3 * n_tiles + 4, 3 * n_tiles + 6)
        last_rows(
            before=lambda: rest(n_tail - 2, n_tail - 1),
            between=lambda: add_parts(3 * n_tiles + 6, 4 * n_tiles - 1),
        )
        add_end(3)
        for u in range(UNITS):
            x1_send(u, vertical).wait_send()
        for u in (2, 3):
            x1_forward(u).wait_send()
        for u in (0, 2, 3):
            each(n_tiles, lambda t: part_copy(u, t).wait_send())
        each(n_tiles - 1, lambda t: part_copy(1, t).wait_send())
        end_copy(1).wait_send()

    each(8, lambda c: far_copy(c).wait_send())


def round_kernel(steps, acc, out, buf, sem):
    height = acc.shape[0] // steps

    def rows_of(s):
        return pl.ds(pl.multiple_of(s * height, height), height)

    def put(s):
        slot = lax.rem(s, R_BUFFERS)
        return pltpu.make_async_copy(buf.at[slot], out.at[rows_of(s)], sem.at[slot])

    def body(s, carry):
        @pl.when(s >= R_BUFFERS)
        def _():
            put(s - R_BUFFERS).wait()

        buf[lax.rem(s, R_BUFFERS)] = acc[rows_of(s), :].astype(out.dtype)
        put(s).start()
        return carry

    lax.fori_loop(0, steps, body, 0)
    for s in range(steps - R_BUFFERS, steps):
        put(jnp.int32(s)).wait()


def rounded(acc):
    rows, cols = acc.shape
    steps = max(rows // R_ROWS, R_BUFFERS)
    return pl.pallas_call(
        functools.partial(round_kernel, steps),
        out_shape=jax.ShapeDtypeStruct((rows, cols), jnp.bfloat16),
        in_specs=[pl.BlockSpec(memory_space=pltpu.VMEM)],
        out_specs=pl.BlockSpec(memory_space=pl.ANY),
        scratch_shapes=[
            pltpu.VMEM((R_BUFFERS, rows // steps, cols), jnp.bfloat16),
            pltpu.SemaphoreType.DMA((R_BUFFERS,)),
        ],
        compiler_params=pltpu.CompilerParams(vmem_limit_bytes=20 * 1024 * 1024),
    )(pltpu.with_memory_space_constraint(acc, pltpu.VMEM))


def solution(mesh):
    grid_spec = P(("dp", "ri", "ro"), "co")

    def local_block(a_block, b_block):
        rows, k_half = a_block.shape
        k_quarter, cols = b_block.shape
        sizes = make_sizes(rows, k_half, cols)
        n_x0 = k_half // sizes["x0_depth"]
        n_tail = k_half // sizes["tail_depth"]
        n_part = UNITS * (cols // sizes["tile"])
        dma = pltpu.SemaphoreType.DMA
        results = pl.pallas_call(
            functools.partial(kernel, sizes),
            out_shape=[
                pltpu.VMEM((rows, cols), jnp.float32),
                jax.ShapeDtypeStruct((k_quarter, cols), jnp.bfloat16),
                jax.ShapeDtypeStruct((rows, k_half), jnp.bfloat16),
                jax.ShapeDtypeStruct((rows, k_half), jnp.bfloat16),
                jax.ShapeDtypeStruct((rows, cols), jnp.float32),
                jax.ShapeDtypeStruct((rows, cols), jnp.float32),
            ],
            in_specs=[pl.BlockSpec(memory_space=pl.ANY)] * 2,
            out_specs=[pl.BlockSpec(memory_space=pltpu.VMEM)] + [pl.BlockSpec(memory_space=pl.ANY)] * 5,
            scratch_shapes=[
                dma((8,)),
                dma((8,)),
                pltpu.VMEM((rows, sizes["tail_depth"]), jnp.bfloat16),
                pltpu.VMEM((sizes["unit"], sizes["tile"]), jnp.float32),
                dma((n_x0 // 2,)),
                dma((n_x0 // 2,)),
                dma((n_tail // 2 - 1,)),
                dma((n_tail // 2 - 1,)),
                dma((UNITS,)),
                dma((UNITS,)),
                dma((UNITS,)),
                dma((UNITS,)),
                dma((UNITS,)),
                dma((n_part,)),
                dma((n_part,)),
                dma,
                dma,
                dma((B_BUFFERS,)),
                dma,
                dma,
            ],
            compiler_params=pltpu.CompilerParams(
                collective_id=0, has_side_effects=True, vmem_limit_bytes=30 * 1024 * 1024
            ),
        )(a_block, b_block)
        return rounded(results[0])

    return jax.shard_map(local_block, mesh=mesh, in_specs=(grid_spec, grid_spec), out_specs=grid_spec, check_vma=False)
```

```python
import functools

import jax
import jax.numpy as jnp
from jax import lax
from jax.experimental import pallas as pl
from jax.experimental.pallas import tpu as pltpu
from jax.sharding import PartitionSpec as P

MESH = pl.DeviceIdType.MESH
UNITS = 4
B_BUFFERS = 3
P_BUFFERS = 4
PIECES = 8
R_BUFFERS = 8
R_ROWS = 32


def make_sizes(rows, k_half, cols):
    k_quarter = k_half // 2
    return dict(
        rows=rows,
        k_half=k_half,
        k_quarter=k_quarter,
        cols=cols,
        unit=rows // UNITS,
        tile=cols // 8,
        x0_depth=k_quarter // 8,
        tail_depth=k_quarter // 16,
        x1_depth=k_quarter // 4,
    )


def kernel(sizes, a, b, acc, b_far, x0, x1, stage, part, far_s, far_r, x_last, part_last, x0_s, x0_r, tail_s, tail_r, last_s, last_r, x1_s, x1_r, fwd_s, part_s, part_r, end_s, end_r, b_sem, x_sem, o_sem):
    rows, k_half, k_quarter = sizes["rows"], sizes["k_half"], sizes["k_quarter"]
    unit, tile = sizes["unit"], sizes["tile"]
    n_tiles = sizes["cols"] // tile
    i, j, r = lax.axis_index("ri"), lax.axis_index("co"), lax.axis_index("ro")
    dp = lax.axis_index("dp")
    vertical, horizontal = (dp, 1 - i, j, r), (dp, i, 1 - j, r)
    opposite, partner = (dp, 1 - i, 1 - j, r), (dp, i, j, 1 - r)
    diag = i == j
    off = jnp.logical_not(diag)

    barrier = pltpu.get_barrier_semaphore()
    for device in (vertical, horizontal, opposite, partner):
        pl.semaphore_signal(barrier, inc=1, device_id=device, device_id_type=MESH)
    pl.semaphore_wait(barrier, 4)

    def remote(src, dst, send, recv, device):
        return pltpu.make_async_remote_copy(
            src_ref=src, dst_ref=dst, send_sem=send, recv_sem=recv, device_id=device, device_id_type=MESH
        )

    far_rows = k_quarter // 8

    def far_copy(c):
        block = pl.ds(c * far_rows, far_rows)
        return remote(b.at[block], b_far.at[block], far_s.at[c], far_r.at[c], partner)

    def k_column(kc, depth):
        return pl.multiple_of(lax.rem(r * k_quarter + kc * depth, k_half), depth)

    def unit_rows(u):
        return pl.ds(pl.multiple_of(u * unit, unit), unit)

    x0_depth, tail_depth = sizes["x0_depth"], sizes["tail_depth"]
    n_x0 = k_half // x0_depth
    n_tail = k_half // tail_depth

    def x0_copy(kc):
        block = pl.ds(k_column(kc, x0_depth), x0_depth)
        return remote(a.at[:, block], x0.at[:, block], x0_s.at[kc], x0_r.at[kc], horizontal)

    def tail_copy(kc):
        block = pl.ds(k_column(kc, tail_depth), tail_depth)
        q = kc - n_tail // 2
        return remote(a.at[:, block], x0.at[:, block], tail_s.at[q], tail_r.at[q], horizontal)

    def piece_rows(q):
        return pl.ds(pl.multiple_of(q * (rows // PIECES), rows // PIECES), rows // PIECES)

    def last_copy(q):
        block = pl.ds(k_column(n_tail - 1, tail_depth), tail_depth)
        return remote(a.at[piece_rows(q), block], x_last.at[piece_rows(q)], last_s.at[q], last_r.at[q], horizontal)

    def x1_send(u, device):
        return remote(a.at[unit_rows(u)], x1.at[unit_rows(u)], x1_s.at[u], x1_r.at[u], device)

    def x1_forward(u):
        return remote(x1.at[unit_rows(u)], x1.at[unit_rows(u)], fwd_s.at[u], x1_r.at[u], horizontal)

    def tile_cols(t):
        return pl.ds(pl.multiple_of(t * tile, tile), tile)

    def part_copy(u, t):
        where = (unit_rows(u), tile_cols(t))
        return remote(stage.at[where], part.at[where], part_s.at[u * n_tiles + t], part_r.at[u * n_tiles + t], vertical)

    def end_copy(u):
        return remote(stage.at[unit_rows(u), tile_cols(n_tiles - 1)], part_last, end_s, end_r, vertical)

    def each(n, step):
        def body(c, carry):
            step(c)
            return carry

        lax.fori_loop(0, n, body, 0)

    def own_rows(first, last, source, b_source, ready=None, b_ready=None, depth=x0_depth):
        far = first * depth >= k_quarter
        base = first - k_quarter // depth if far else first
        steps = (last - first) * n_tiles

        def scope(xbuf, bbuf):
            def b_copy(s):
                c = lax.div(s, n_tiles)
                t = lax.rem(s, n_tiles)
                slot = lax.rem(s, B_BUFFERS)
                k_rows = pl.ds(pl.multiple_of((base + c) * depth, depth), depth)
                return pltpu.make_async_copy(b_source.at[k_rows, tile_cols(t)], bbuf.at[slot], b_sem.at[slot])

            def b_start(s):
                if b_ready is not None:

                    @pl.when(lax.rem(s, n_tiles) == 0)
                    def _():
                        b_ready(base + lax.div(s, n_tiles))

                b_copy(s).start()

            for s in range(B_BUFFERS - 1):
                b_start(jnp.int32(s))

            def body(s, carry):
                c = lax.div(s, n_tiles)
                t = lax.rem(s, n_tiles)

                @pl.when(s + B_BUFFERS - 1 < steps)
                def _():
                    b_start(s + B_BUFFERS - 1)

                @pl.when(t == 0)
                def _():
                    if ready is not None:
                        ready(first + c)
                    block = pl.ds(k_column(first + c, depth), depth)
                    copy = pltpu.make_async_copy(source.at[:, block], xbuf, x_sem)
                    copy.start()
                    copy.wait()

                b_copy(s).wait()
                product = jnp.dot(xbuf[...], bbuf[lax.rem(s, B_BUFFERS)], preferred_element_type=jnp.float32)
                if first == 0:

                    @pl.when(c == 0)
                    def _():
                        acc[:, tile_cols(t)] = product

                    @pl.when(c > 0)
                    def _():
                        acc[:, tile_cols(t)] += product
                else:
                    acc[:, tile_cols(t)] += product
                return carry

            lax.fori_loop(0, steps, body, 0)

        pl.run_scoped(
            scope,
            pltpu.VMEM((rows, depth), jnp.bfloat16),
            pltpu.VMEM((B_BUFFERS, depth, tile), jnp.bfloat16),
        )

    x1_depth = sizes["x1_depth"]
    n_x1 = k_half // x1_depth

    def other_rows(u, final=False):
        steps = n_tiles * n_x1

        def scope(xbuf, bbuf, pbuf):
            def b_start(s):
                t = lax.div(s, n_x1)
                kc = lax.rem(s, n_x1)
                slot = lax.rem(s, B_BUFFERS)

                @pl.when(kc < n_x1 // 2)
                def _():
                    k_rows = pl.ds(pl.multiple_of(kc * x1_depth, x1_depth), x1_depth)
                    pltpu.make_async_copy(b.at[k_rows, tile_cols(t)], bbuf.at[slot], b_sem.at[slot]).start()

                @pl.when(kc >= n_x1 // 2)
                def _():
                    k_rows = pl.ds(pl.multiple_of((kc - n_x1 // 2) * x1_depth, x1_depth), x1_depth)
                    pltpu.make_async_copy(b_far.at[k_rows, tile_cols(t)], bbuf.at[slot], b_sem.at[slot]).start()

            load = pltpu.make_async_copy(x1.at[unit_rows(u)], xbuf, x_sem)
            load.start()
            for s in range(B_BUFFERS - 1):
                b_start(jnp.int32(s))
            load.wait()

            def body(s, carry):
                t = lax.div(s, n_x1)
                kc = lax.rem(s, n_x1)
                slot = lax.rem(s, B_BUFFERS)

                @pl.when(s + B_BUFFERS - 1 < steps)
                def _():
                    b_start(s + B_BUFFERS - 1)

                pltpu.make_async_copy(b.at[pl.ds(0, x1_depth), pl.ds(0, tile)], bbuf.at[slot], b_sem.at[slot]).wait()
                columns = pl.ds(k_column(kc, x1_depth), x1_depth)
                product = jnp.dot(xbuf[:, columns], bbuf[slot], preferred_element_type=jnp.float32)

                @pl.when(kc == 0)
                def _():
                    pbuf[...] = product

                @pl.when(kc > 0)
                def _():
                    pbuf[...] += product

                @pl.when(kc == n_x1 - 1)
                def _():
                    put = pltpu.make_async_copy(pbuf, stage.at[unit_rows(u), tile_cols(t)], o_sem)
                    put.start()
                    put.wait()
                    if final:

                        @pl.when(t < n_tiles - 1)
                        def _():
                            part_copy(u, t).start()

                        @pl.when(t == n_tiles - 1)
                        def _():
                            end_copy(u).start()
                    else:
                        part_copy(u, t).start()

                return carry

            lax.fori_loop(0, steps, body, 0)

        pl.run_scoped(
            scope,
            pltpu.VMEM((unit, k_half), jnp.bfloat16),
            pltpu.VMEM((B_BUFFERS, x1_depth, tile), jnp.bfloat16),
            pltpu.VMEM((unit, tile), jnp.float32),
        )

    def add_parts(first, last, depth=P_BUFFERS):
        depth = min(depth, last - first)

        def scope(pbuf, p_sem):
            def fetch(s):
                where = (unit_rows(lax.div(s, n_tiles)), tile_cols(lax.rem(s, n_tiles)))
                slot = lax.rem(s, P_BUFFERS)
                return pltpu.make_async_copy(part.at[where], pbuf.at[slot], p_sem.at[slot])

            def start(s):
                part_copy(lax.div(s, n_tiles), lax.rem(s, n_tiles)).wait_recv()
                fetch(s).start()

            for s in range(first, first + depth - 1):
                start(jnp.int32(s))

            def body(s, carry):
                @pl.when(s + depth - 1 < last)
                def _():
                    start(s + depth - 1)

                fetch(s).wait()
                acc[unit_rows(lax.div(s, n_tiles)), tile_cols(lax.rem(s, n_tiles))] += pbuf[lax.rem(s, P_BUFFERS)]
                return carry

            lax.fori_loop(first, last, body, 0)

        pl.run_scoped(
            scope,
            pltpu.VMEM((P_BUFFERS, unit, tile), jnp.float32),
            pltpu.SemaphoreType.DMA((P_BUFFERS,)),
        )

    def add_end(u):
        end_copy(u).wait_recv()
        acc[unit_rows(u), tile_cols(n_tiles - 1)] += part_last[...]

    def last_rows(before, between):
        def scope(bbuf):
            load = pltpu.make_async_copy(b_far.at[pl.ds(k_quarter - tail_depth, tail_depth)], bbuf, o_sem)
            load.start()
            before()
            load.wait()

            def step(q):
                last_copy(q).wait_recv()
                for t in range(n_tiles):
                    columns = pl.ds(t * tile, tile)
                    acc[piece_rows(q), columns] += jnp.dot(
                        x_last[piece_rows(q), :], bbuf[:, columns], preferred_element_type=jnp.float32
                    )

            each(PIECES - 1, step)
            between()
            each(1, lambda q: step(q + PIECES - 1))

        pl.run_scoped(scope, pltpu.VMEM((tail_depth, sizes["cols"]), jnp.bfloat16))

    half = n_x0 // 2
    quarter = n_x0 // 4
    thin = n_tail // 2

    @pl.when(diag)
    def _():
        each(half, lambda c: x0_copy(c).start())
        each(8, lambda c: far_copy(c).start())
        own_rows(0, half, a, b)
        own_rows(half, n_x0 - 2, a, b_far, b_ready=lambda c: far_copy(c).wait_recv())
        for c in (6, 7):
            far_copy(c).wait_recv()
        x1_forward(0).wait_recv()
        x1_forward(0).start()
        other_rows(0)
        x1_forward(1).wait_recv()
        x1_forward(1).start()
        each(thin - 1, lambda c: tail_copy(thin + c).start())
        each(PIECES, lambda q: last_copy(q).start())
        own_rows(n_x0 - 2, n_x0, a, b_far)
        other_rows(1)
        for u in (2, 3):
            x1_forward(u).wait_recv()
            other_rows(u, final=u == 3)
        add_parts(2 * n_tiles, 4 * n_tiles)
        add_parts(0, n_tiles)
        add_parts(n_tiles, 2 * n_tiles - 1, depth=1)
        add_end(1)
        each(half, lambda c: x0_copy(c).wait_send())
        each(thin - 1, lambda c: tail_copy(thin + c).wait_send())
        each(PIECES, lambda q: last_copy(q).wait_send())
        for u in (0, 1):
            x1_forward(u).wait_send()
        for u in (0, 1, 2):
            each(n_tiles, lambda t: part_copy(u, t).wait_send())
        each(n_tiles - 1, lambda t: part_copy(3, t).wait_send())
        end_copy(3).wait_send()

    @pl.when(off)
    def _():
        for u in (0, 1):
            x1_send(u, vertical).start()
        for u in (2, 3):
            x1_send(u, opposite).start()
        each(8, lambda c: far_copy(c).start())
        arrived = lambda c: x0_copy(c).wait_recv()
        own_rows(0, quarter, x0, b, ready=arrived)
        x1_forward(2).wait_recv()
        x1_forward(2).start()
        each(8, lambda c: far_copy(c).wait_recv())
        other_rows(2)
        own_rows(quarter, half, x0, b, ready=arrived)
        x1_forward(3).wait_recv()
        x1_forward(3).start()
        other_rows(3)
        for u in (0, 1):
            x1_forward(u).wait_recv()
            other_rows(u, final=u == 1)
        thin_arrived = lambda c: tail_copy(c).wait_recv()
        rest = lambda first, last: own_rows(first, last, x0, b_far, ready=thin_arrived, depth=tail_depth)
        rest(thin, thin + 8)
        add_parts(0, 2 * n_tiles)
        rest(thin + 8, n_tail - 4)
        add_parts(2 * n_tiles, 3 * n_tiles + 4)
        rest(n_tail - 4, n_tail - 2)
        add_parts(3 * n_tiles + 4, 3 * n_tiles + 6)
        last_rows(
            before=lambda: rest(n_tail - 2, n_tail - 1),
            between=lambda: add_parts(3 * n_tiles + 6, 4 * n_tiles - 1),
        )
        add_end(3)
        for u in range(UNITS):
            x1_send(u, vertical).wait_send()
        for u in (2, 3):
            x1_forward(u).wait_send()
        for u in (0, 2, 3):
            each(n_tiles, lambda t: part_copy(u, t).wait_send())
        each(n_tiles - 1, lambda t: part_copy(1, t).wait_send())
        end_copy(1).wait_send()

    each(8, lambda c: far_copy(c).wait_send())


def round_kernel(steps, acc, out, buf, sem):
    height = acc.shape[0] // steps

    def rows_of(s):
        return pl.ds(pl.multiple_of(s * height, height), height)

    def put(s):
        slot = lax.rem(s, R_BUFFERS)
        return pltpu.make_async_copy(buf.at[slot], out.at[rows_of(s)], sem.at[slot])

    def body(s, carry):
        @pl.when(s >= R_BUFFERS)
        def _():
            put(s - R_BUFFERS).wait()

        buf[lax.rem(s, R_BUFFERS)] = acc[rows_of(s), :].astype(out.dtype)
        put(s).start()
        return carry

    lax.fori_loop(0, steps, body, 0)
    for s in range(steps - R_BUFFERS, steps):
        put(jnp.int32(s)).wait()


def rounded(acc):
    rows, cols = acc.shape
    steps = max(rows // R_ROWS, R_BUFFERS)
    return pl.pallas_call(
        functools.partial(round_kernel, steps),
        out_shape=jax.ShapeDtypeStruct((rows, cols), jnp.bfloat16),
        in_specs=[pl.BlockSpec(memory_space=pltpu.VMEM)],
        out_specs=pl.BlockSpec(memory_space=pl.ANY),
        scratch_shapes=[
            pltpu.VMEM((R_BUFFERS, rows // steps, cols), jnp.bfloat16),
            pltpu.SemaphoreType.DMA((R_BUFFERS,)),
        ],
        compiler_params=pltpu.CompilerParams(vmem_limit_bytes=20 * 1024 * 1024),
    )(pltpu.with_memory_space_constraint(acc, pltpu.VMEM))


def solution(mesh):
    grid_spec = P(("dp", "ri", "ro"), "co")

    def local_block(a_block, b_block):
        rows, k_half = a_block.shape
        k_quarter, cols = b_block.shape
        sizes = make_sizes(rows, k_half, cols)
        n_x0 = k_half // sizes["x0_depth"]
        n_tail = k_half // sizes["tail_depth"]
        n_part = UNITS * (cols // sizes["tile"])
        dma = pltpu.SemaphoreType.DMA
        results = pl.pallas_call(
            functools.partial(kernel, sizes),
            out_shape=[
                pltpu.VMEM((rows, cols), jnp.float32),
                jax.ShapeDtypeStruct((k_quarter, cols), jnp.bfloat16),
                jax.ShapeDtypeStruct((rows, k_half), jnp.bfloat16),
                jax.ShapeDtypeStruct((rows, k_half), jnp.bfloat16),
                jax.ShapeDtypeStruct((rows, cols), jnp.float32),
                jax.ShapeDtypeStruct((rows, cols), jnp.float32),
            ],
            in_specs=[pl.BlockSpec(memory_space=pl.ANY)] * 2,
            out_specs=[pl.BlockSpec(memory_space=pltpu.VMEM)] + [pl.BlockSpec(memory_space=pl.ANY)] * 5,
            scratch_shapes=[
                dma((8,)),
                dma((8,)),
                pltpu.VMEM((rows, sizes["tail_depth"]), jnp.bfloat16),
                pltpu.VMEM((sizes["unit"], sizes["tile"]), jnp.float32),
                dma((n_x0 // 2,)),
                dma((n_x0 // 2,)),
                dma((n_tail // 2 - 1,)),
                dma((n_tail // 2 - 1,)),
                dma((PIECES,)),
                dma((PIECES,)),
                dma((UNITS,)),
                dma((UNITS,)),
                dma((UNITS,)),
                dma((n_part,)),
                dma((n_part,)),
                dma,
                dma,
                dma((B_BUFFERS,)),
                dma,
                dma,
            ],
            compiler_params=pltpu.CompilerParams(
                collective_id=0, has_side_effects=True, vmem_limit_bytes=30 * 1024 * 1024
            ),
        )(a_block, b_block)
        return rounded(results[0])

    return jax.shard_map(local_block, mesh=mesh, in_specs=(grid_spec, grid_spec), out_specs=grid_spec, check_vma=False)
```
